256 devices in a mesh: groups: 2 (over y), ctx: 128 (over x, z, core).
Axes of the slice: x: 4, y: 2, z: 16, core: 2. Of those that a mesh axis runs over, the one named last changes fastest.
The devices are a block of a 4x16x16 slice.
Arguments:
- prompt_query: bfloat16 [16384, 4096], P(('groups', 'ctx')), parts along dimension 0, may hold values from -6 to 6
- prompt_key: bfloat16 [16384, 512], P(('groups', 'ctx')), parts along dimension 0, may hold values from -6 to 6
- prompt_value: bfloat16 [16384, 512], P(('groups', 'ctx')), parts along dimension 0, may hold values from -6 to 6
- prefix_key_cache: bfloat16 [2048, 512], P(('groups', 'ctx')), parts along dimension 0, may hold values from -6 to 6
- prefix_value_cache: bfloat16 [2048, 512], P(('groups', 'ctx')), parts along dimension 0, may hold values from -6 to 6
- decoded_query: bfloat16 [8192], P('groups'), parts along dimension 0, may hold values from -6 to 6
- decoded_key: bfloat16 [1024], P('groups'), parts along dimension 0, may hold values from -6 to 6
- decoded_value: bfloat16 [1024], P('groups'), parts along dimension 0, may hold values from -6 to 6
- shard_counts: int32 [256, 2], P('groups'), parts along dimension 0, may hold values from 0 to 32, as said below
- block_offsets: int32 [256, 2], P('groups'), parts along dimension 0, may hold values from 0 to 8160, as said below
Outputs:
- span_out: bfloat16 [16384, 4096], P(('groups', 'ctx')), parts along dimension 0
- next_out: bfloat16 [8192], P('groups'), parts along dimension 0
The draws below stay inside these ranges and needn't reach their ends.
There are 2 independent parts, one for each index of `groups`. The reference program is written for one: setup_inputs(seed, part) draws one part's arguments, and reference() takes and returns one part's arrays. A program takes and returns all parts, laid end to end along the dimension named above; each array names one. Nothing has to cross between parts.
Inputs may be any that keep to these rules, and one draw needn't show every extreme that they name: block_offsets[i, 0] = 32 * p_i and block_offsets[i, 1] = 32 * (255 - p_i) for a permutation p of 0 to 127. shard_counts[i, h] = min(32, max(0, L - block_offsets[i, h])) for one prompt length L with 4096 < L <= 8128.
All inputs are finite; a program needn't handle non-finite values.
Results may differ from the reference program's by a relative error of at most 0.0055.
Values may be sent and summed in bfloat16 or wider, within the bound.
No kernel may reach another device: no remote copies, remote signals or barrier semaphores. Data moves between devices by JAX's collectives and lax.ppermute only.
A program may use at most 128 MiB of HBM per device.

```python
import jax
import jax.numpy as jnp
from jax import lax

QUERY_HEADS = 32
KEY_VALUE_HEADS = 4
HEAD_WIDTH = 128
HEADS_PER_GROUP = 8
T_DEV = 64
C_DEV = 8
HALF = 32
PROMPT_SLOTS = 8192
PREFIX_LENGTH = 1024
N_CTX = 128


def flipped_signs(key):
    random_flip_bits = jax.random.randint(jax.random.fold_in(key, 11), (KEY_VALUE_HEADS, HEAD_WIDTH), 0, 2)
    return (2 * random_flip_bits - 1).astype(jnp.float32)


def draw_prompt_query(key, part):
    value_matrix = jax.random.truncated_normal(jax.random.fold_in(key, 1), -6.0, 6.0, (PROMPT_SLOTS, QUERY_HEADS * HEAD_WIDTH), jnp.float32)
    random_sign_rows = jnp.repeat(flipped_signs(key), QUERY_HEADS // KEY_VALUE_HEADS, axis=0).reshape(QUERY_HEADS * HEAD_WIDTH)
    chosen = jax.random.randint(jax.random.fold_in(key, 2), (PROMPT_SLOTS,), 0, 32)
    levels = jax.random.randint(jax.random.fold_in(key, 3), (PROMPT_SLOTS,), 3, 7).astype(jnp.float32)
    value_matrix = jnp.where((chosen == 0)[:, None], levels[:, None] * random_sign_rows[None, :], value_matrix)
    return value_matrix.astype(jnp.bfloat16)


def draw_prefix_key_cache(key, part):
    value_matrix = jax.random.truncated_normal(jax.random.fold_in(key, 4), -6.0, 6.0, (PREFIX_LENGTH, KEY_VALUE_HEADS * HEAD_WIDTH), jnp.float32)
    random_sign_rows = flipped_signs(key).reshape(KEY_VALUE_HEADS * HEAD_WIDTH)
    hot_first = C_DEV + jax.random.randint(jax.random.fold_in(key, 5), (), 0, C_DEV)
    hot_second = C_DEV * (N_CTX // 2) + jax.random.randint(jax.random.fold_in(key, 6), (), 0, C_DEV)
    row_ids = jnp.arange(PREFIX_LENGTH)
    value_matrix = jnp.where((row_ids == hot_first)[:, None], 5.0 * random_sign_rows[None, :], value_matrix)
    value_matrix = jnp.where((row_ids == hot_second)[:, None], 5.0625 * random_sign_rows[None, :], value_matrix)
    return value_matrix.astype(jnp.bfloat16)


def decode_pair(key):
    random_sign_rows = flipped_signs(key)
    single_query_row = 4.0 * jnp.repeat(random_sign_rows, QUERY_HEADS // KEY_VALUE_HEADS, axis=0).reshape(QUERY_HEADS * HEAD_WIDTH)
    single_key_row = 5.0625 * random_sign_rows.reshape(KEY_VALUE_HEADS * HEAD_WIDTH)
    return (single_query_row, single_key_row)


def draw_decoded_query(key, part):
    return decode_pair(key)[0].astype(jnp.bfloat16)


def draw_decoded_key(key, part):
    return decode_pair(key)[1].astype(jnp.bfloat16)


def span_layout(key):
    ordering = jax.random.permutation(jax.random.fold_in(key, 21), N_CTX)
    starts = jnp.stack([ordering * HALF, (2 * N_CTX - 1 - ordering) * HALF], axis=1)
    prompt_len = jax.random.randint(jax.random.fold_in(key, 22), (), PROMPT_SLOTS // 2 + 1, PROMPT_SLOTS - T_DEV + 1)
    counts = jnp.clip(prompt_len - starts, 0, HALF)
    return (starts.astype(jnp.int32), counts.astype(jnp.int32))


def draw_block_offsets(key, part):
    return span_layout(key)[0]


def draw_shard_counts(key, part):
    return span_layout(key)[1]


def shard_levels(rng, extent, split, least, high):
    level, own = 1.0, jax.random.fold_in(rng, 6)
    for dim, blocks in split:
        draws = jnp.exp(jax.random.uniform(jax.random.fold_in(own, dim), (blocks,), jnp.float32, least / len(split), high / len(split)))
        level = level * jnp.repeat(draws, extent[dim] // blocks).reshape([-1 if axis == dim else 1 for axis in range(len(extent))])
    return level


def gaussian(own_key, dims, spread, limit, split=(), kind=jnp.bfloat16):
    gain = shard_levels(own_key, dims, split, -0.22, 0.18) if split else 1.0
    result = jax.random.normal(own_key, dims, jnp.float32) * spread * gain
    return jnp.minimum(jnp.maximum(result, -limit), limit).astype(kind)


def setup_inputs(seed: int = 0, part: int = 0) -> dict:
    arg_keys = jax.random.split(jax.random.key(seed), 11)
    own_keys = jax.random.split(jax.random.fold_in(arg_keys[10], part), 11)
    prompt_query = draw_prompt_query(jax.random.fold_in(jax.random.fold_in(arg_keys[10], part), 71), part)
    prompt_key = gaussian(own_keys[1], (PROMPT_SLOTS, KEY_VALUE_HEADS * HEAD_WIDTH), 1.0, 6.0, ((0, 128),))
    prompt_value = gaussian(own_keys[2], (PROMPT_SLOTS, KEY_VALUE_HEADS * HEAD_WIDTH), 1.0, 6.0, ((0, 128),))
    prefix_key_cache = draw_prefix_key_cache(jax.random.fold_in(jax.random.fold_in(arg_keys[10], part), 71), part)
    prefix_value_cache = gaussian(own_keys[4], (PREFIX_LENGTH, KEY_VALUE_HEADS * HEAD_WIDTH), 1.0, 6.0, ((0, 128),))
    decoded_query = draw_decoded_query(jax.random.fold_in(jax.random.fold_in(arg_keys[10], part), 71), part)
    decoded_key = draw_decoded_key(jax.random.fold_in(jax.random.fold_in(arg_keys[10], part), 71), part)
    decoded_value = gaussian(own_keys[7], (KEY_VALUE_HEADS * HEAD_WIDTH,), 1.0, 6.0)
    shard_counts = draw_shard_counts(jax.random.fold_in(jax.random.fold_in(arg_keys[10], part), 71), part)
    block_offsets = draw_block_offsets(jax.random.fold_in(jax.random.fold_in(arg_keys[10], part), 71), part)
    return dict(prompt_query=prompt_query, prompt_key=prompt_key, prompt_value=prompt_value, prefix_key_cache=prefix_key_cache, prefix_value_cache=prefix_value_cache, decoded_query=decoded_query, decoded_key=decoded_key, decoded_value=decoded_value, shard_counts=shard_counts, block_offsets=block_offsets)


def slot_layout(shard_counts, block_offsets):
    slot_ids = jnp.arange(PROMPT_SLOTS, dtype=jnp.int32)
    shard_ids = slot_ids // T_DEV
    within = slot_ids % T_DEV
    piece_ids = within // HALF
    offset_in = within % HALF
    position = PREFIX_LENGTH + block_offsets[shard_ids, piece_ids] + offset_in
    is_live = offset_in < shard_counts[shard_ids, piece_ids]
    return position.astype(jnp.int32), is_live


def reference(prompt_query, prompt_key, prompt_value, prefix_key_cache, prefix_value_cache, decoded_query, decoded_key, decoded_value, shard_counts, block_offsets):
    logit_scale = HEAD_WIDTH ** -0.5
    position, is_live = slot_layout(shard_counts, block_offsets)
    key_pos = jnp.concatenate([jnp.arange(PREFIX_LENGTH, dtype=jnp.int32), position])
    key_live = jnp.concatenate([jnp.ones((PREFIX_LENGTH,), dtype=bool), is_live])
    head_key_rows = jnp.concatenate([prefix_key_cache, prompt_key], 0).astype(jnp.float32).reshape(-1, KEY_VALUE_HEADS, HEAD_WIDTH)
    head_value_rows = jnp.concatenate([prefix_value_cache, prompt_value], 0).astype(jnp.float32).reshape(-1, KEY_VALUE_HEADS, HEAD_WIDTH)
    prompt_block_rows = 128 if PROMPT_SLOTS % 128 == 0 else PROMPT_SLOTS

    def one_block(block_item):
        query_rows, query_pos, query_live = block_item
        query_head_list = query_rows.astype(jnp.float32).reshape(prompt_block_rows, KEY_VALUE_HEADS, HEADS_PER_GROUP, HEAD_WIDTH)
        scores = jnp.einsum("tgqd,rgd->tgqr", query_head_list, head_key_rows) * logit_scale
        visible = key_live[None, :] & (key_pos[None, :] <= query_pos[:, None])
        scores = jnp.where(visible[:, None, None, :], scores, -jnp.inf)
        peaks = jnp.max(scores, axis=-1, keepdims=True)
        weights = jnp.exp(scores - peaks)
        totals = jnp.sum(weights, axis=-1)
        rounded = lax.optimization_barrier(weights.astype(jnp.bfloat16)).astype(jnp.float32)
        value_mixture = jnp.einsum("tgqr,rgd->tgqd", rounded, head_value_rows) / totals[..., None]
        value_mixture = jnp.where(query_live[:, None, None, None], value_mixture, 0.0)
        return value_mixture.reshape(prompt_block_rows, QUERY_HEADS * HEAD_WIDTH).astype(jnp.bfloat16)

    outputs = lax.map(one_block, (prompt_query.reshape(PROMPT_SLOTS // prompt_block_rows, prompt_block_rows, QUERY_HEADS * HEAD_WIDTH), position.reshape(-1, prompt_block_rows), is_live.reshape(-1, prompt_block_rows)))
    span_out = outputs.reshape(PROMPT_SLOTS, QUERY_HEADS * HEAD_WIDTH)

    decoded_query_row = decoded_query.astype(jnp.float32).reshape(KEY_VALUE_HEADS, HEADS_PER_GROUP, HEAD_WIDTH)
    next_scores = jnp.einsum("gqd,rgd->gqr", decoded_query_row, head_key_rows) * logit_scale
    next_scores = jnp.where(key_live[None, None, :], next_scores, -jnp.inf)
    self_score = jnp.einsum("sop,sp->so", decoded_query_row, decoded_key.astype(jnp.float32).reshape(KEY_VALUE_HEADS, HEAD_WIDTH)) * logit_scale
    peaks = jnp.maximum(jnp.max(next_scores, axis=-1), self_score)
    next_weights = jnp.exp(next_scores - peaks[..., None])
    self_weight = jnp.exp(self_score - peaks)
    totals = jnp.sum(next_weights, axis=-1) + self_weight
    rounded = lax.optimization_barrier(next_weights.astype(jnp.bfloat16)).astype(jnp.float32)
    value_mixture = jnp.einsum("gqr,rgd->gqd", rounded, head_value_rows)
    value_mixture = value_mixture + self_weight[..., None] * decoded_value.astype(jnp.float32).reshape(KEY_VALUE_HEADS, 1, HEAD_WIDTH)
    next_out = (value_mixture / totals[..., None]).reshape(QUERY_HEADS * HEAD_WIDTH).astype(jnp.bfloat16)
    return (span_out, next_out)
```

```python
import functools

import jax
import jax.numpy as jnp
from jax import lax
from jax.experimental import pallas as pl
from jax.experimental.pallas import tpu as pltpu
from jax.sharding import Mesh
from jax.sharding import PartitionSpec as P

KEY_VALUE_HEADS = 4
HEAD_WIDTH = 128
HEADS_PER_GROUP = 8
GROUP_WIDTH = HEADS_PER_GROUP * HEAD_WIDTH
CTX = ("ctx_0", "ctx_1", "ctx_2")
GROUPS_CTX = ("groups", "ctx_0", "ctx_1", "ctx_2")
RING = ("ctx_1", "ctx_2")
COLUMNS = KEY_VALUE_HEADS
CORES = 2
HALF = 32
PREFIX = 8
LOW = COLUMNS * HALF
NEAR = LOW + COLUMNS * PREFIX
BLOCK = NEAR + LOW
TILES = 2 * COLUMNS
TILE = HALF * HEADS_PER_GROUP
NEGATIVE_FILL = -1e30
EXP2_SCALE = HEAD_WIDTH**-0.5 * 1.4426950408889634
NT = (((1,), (1,)), ((), ()))


def source_index(where_ref, column, ring_step, flip, depth):
    x, z, core = where_ref[0], where_ref[1], where_ref[2]
    way = jnp.where(core == 0, -ring_step, ring_step)
    if flip[0]:
        way = -way
    z_from = lax.rem(z + way + depth, depth)
    core_from = 1 - core if flip[1] else core
    x_from = lax.rem(x - column + COLUMNS, COLUMNS)
    return (x_from * depth + z_from) * CORES + core_from


def attention_step(
    where_ref, offset_ref, count_ref, *refs, ring_step, flips, depth, first, last
):
    blocks = refs[: len(flips)]
    refs = refs[len(flips) :]
    query_ref, decode_query_ref = refs[:2]
    refs = refs[2:]
    if last:
        decode_key_ref, decode_value_ref = refs[:2]
        refs = refs[2:]
    if not first:
        acc_in, stats_in, decode_in = refs[:3]
        refs = refs[3:]
    if last:
        out_ref = refs[0]
        refs = refs[1:]
    else:
        acc_out, stats_out, decode_out = refs[:3]
        refs = refs[3:]
    keys, values_t, score_ref, weight_ref = refs

    count = len(flips)
    near, total = count * NEAR, count * BLOCK
    for b, block in enumerate(blocks):
        keys[b * NEAR : (b + 1) * NEAR, :] = block[:NEAR, :HEAD_WIDTH]
        keys[near + b * LOW : near + (b + 1) * LOW, :] = block[NEAR:, :HEAD_WIDTH]
    values = jnp.concatenate(
        [block[:NEAR, HEAD_WIDTH:] for block in blocks]
        + [block[NEAR:, HEAD_WIDTH:] for block in blocks],
        0,
    )
    values_t[...] = values.T

    spread = lax.broadcasted_iota(jnp.int32, (HALF, TILE), 0) - lax.rem(
        lax.broadcasted_iota(jnp.int32, (HALF, TILE), 1), HALF
    )
    sources = [
        [source_index(where_ref, j, ring_step, flip, depth) for j in range(COLUMNS)]
        for flip in flips
    ]

    def tile_step(column, half):
        tile = column * 2 + half
        rows = total if half else near
        query = jnp.concatenate(
            [
                query_ref[column, half * HALF : (half + 1) * HALF, h * HEAD_WIDTH : (h + 1) * HEAD_WIDTH]
                for h in range(HEADS_PER_GROUP)
            ],
            0,
        )
        score_ref[:rows, :] = lax.dot_general(
            keys[:rows, :], query, NT, preferred_element_type=jnp.float32
        )
        own = source_index(where_ref, column, 0, (False, False), depth)
        query_base = offset_ref[own * 2 + half]
        for b in range(count):
            for j in range(COLUMNS):
                at = (near + b * LOW if half else b * NEAR) + j * HALF
                gap = query_base - offset_ref[sources[b][j] * 2 + half]
                score_ref[at : at + HALF, :] = jnp.where(
                    spread <= gap, score_ref[at : at + HALF, :], NEGATIVE_FILL
                )
        peak = jnp.max(score_ref[:rows, :], axis=0, keepdims=True)
        if not first:
            old_peak = stats_in[tile, 0:1, :]
            peak = jnp.maximum(peak, old_peak)
        weights = jnp.exp2((score_ref[:rows, :] - peak) * EXP2_SCALE)
        weight_ref[:rows, :] = weights.astype(jnp.bfloat16)
        totals = jnp.sum(weights, axis=0, keepdims=True)
        mixture = jnp.dot(
            values_t[:, :rows], weight_ref[:rows, :], preferred_element_type=jnp.float32
        )
        if not first:
            rescale = jnp.exp2((old_peak - peak) * EXP2_SCALE)
            totals = totals + rescale * stats_in[tile, 1:2, :]
            mixture = mixture + rescale * acc_in[tile]
        if last:
            live = count_ref[own * 2 + half]
            slot = lax.rem(lax.broadcasted_iota(jnp.int32, (1, TILE), 1), HALF)
            factor = jnp.where(slot < live, 1.0 / totals, 0.0)
            result = (mixture * factor).T.astype(jnp.bfloat16)
            for h in range(HEADS_PER_GROUP):
                out_ref[column, half * HALF : (half + 1) * HALF, h * HEAD_WIDTH : (h + 1) * HEAD_WIDTH] = (
                    result[h * HALF : (h + 1) * HALF, :]
                )
        else:
            acc_out[tile] = mixture
            stats_out[tile, 0:1, :] = peak
            stats_out[tile, 1:2, :] = totals

    def both(column, carry):
        tile_step(column, 0)
        tile_step(column, 1)
        return carry

    lax.fori_loop(0, COLUMNS, both, 0)

    scores = lax.dot_general(
        decode_query_ref[...], keys[...], NT, preferred_element_type=jnp.float32
    )
    lane = lax.broadcasted_iota(jnp.int32, (1, total), 1)
    live = jnp.full((1, total), HALF, jnp.int32)
    for b in range(count):
        for j in range(COLUMNS):
            at = near + b * LOW + j * HALF
            live = jnp.where(
                (lane >= at) & (lane < at + HALF), count_ref[sources[b][j] * 2 + 1], live
            )
    scores = jnp.where(lax.rem(lane, HALF) < live, scores, NEGATIVE_FILL)
    peak = jnp.max(scores, axis=1, keepdims=True)
    if not first:
        old_peak = decode_in[:, HEAD_WIDTH : HEAD_WIDTH + 1]
        peak = jnp.maximum(peak, old_peak)
    weights = jnp.exp2((scores - peak) * EXP2_SCALE)
    totals = jnp.sum(weights, axis=1, keepdims=True)
    mixture = lax.dot_general(
        weights.astype(jnp.bfloat16), values_t[...], NT, preferred_element_type=jnp.float32
    )
    if not first:
        rescale = jnp.exp2((old_peak - peak) * EXP2_SCALE)
        totals = totals + rescale * decode_in[:, 2 * HEAD_WIDTH : 2 * HEAD_WIDTH + 1]
        mixture = mixture + rescale * decode_in[:, :HEAD_WIDTH]
    if last:
        query = decode_query_ref[...].astype(jnp.float32)
        own_score = jnp.sum(
            query * decode_key_ref[...].astype(jnp.float32), axis=1, keepdims=True
        )
        top = jnp.maximum(peak, own_score)
        keep = jnp.exp2((peak - top) * EXP2_SCALE)
        own_weight = jnp.exp2((own_score - top) * EXP2_SCALE)
        numerator = keep * mixture + own_weight * decode_value_ref[...].astype(jnp.float32)
        result = numerator / (keep * totals + own_weight)
        for column in range(COLUMNS):
            for h in range(HEADS_PER_GROUP):
                out_ref[column, 2 * HALF : 2 * HALF + 8, h * HEAD_WIDTH : (h + 1) * HEAD_WIDTH] = (
                    jnp.broadcast_to(result[h : h + 1, :], (8, HEAD_WIDTH)).astype(jnp.bfloat16)
                )
    else:
        decode_out[:, :HEAD_WIDTH] = mixture
        decode_out[:, HEAD_WIDTH : 2 * HEAD_WIDTH] = jnp.broadcast_to(peak, mixture.shape)
        decode_out[:, 2 * HEAD_WIDTH :] = jnp.broadcast_to(totals, mixture.shape)


STATE = (
    jax.ShapeDtypeStruct((TILES, HEAD_WIDTH, TILE), jnp.float32),
    jax.ShapeDtypeStruct((TILES, 8, TILE), jnp.float32),
    jax.ShapeDtypeStruct((16, 3 * HEAD_WIDTH), jnp.float32),
)


def run_step(where, offsets, counts, blocks, flips, ring_step, depth, query, decode, state, last):
    first = state is None
    smem = pl.BlockSpec(memory_space=pltpu.SMEM)
    vmem = pl.BlockSpec(memory_space=pltpu.VMEM)
    operands = [where, offsets, counts, *blocks, query, decode[0]]
    if last:
        operands += decode[1:]
    aliases = {}
    if not first:
        if not last:
            aliases = {len(operands) + i: i for i in range(3)}
        operands += state
    total = len(blocks) * BLOCK
    if last:
        out_shape = jax.ShapeDtypeStruct((COLUMNS, 2 * HALF + 8, GROUP_WIDTH), jnp.bfloat16)
        out_specs = vmem
    else:
        out_shape, out_specs = STATE, (vmem,) * 3
    kernel = functools.partial(
        attention_step, ring_step=ring_step, flips=flips, depth=depth, first=first, last=last
    )
    return pl.pallas_call(
        kernel,
        out_shape=out_shape,
        in_specs=[smem] * 3 + [vmem] * (len(operands) - 3),
        out_specs=out_specs,
        scratch_shapes=[
            pltpu.VMEM((total, HEAD_WIDTH), jnp.bfloat16),
            pltpu.VMEM((HEAD_WIDTH, total), jnp.bfloat16),
            pltpu.VMEM((total, TILE), jnp.float32),
            pltpu.VMEM((total, TILE), jnp.bfloat16),
        ],
        input_output_aliases=aliases,
        compiler_params=pltpu.CompilerParams(vmem_limit_bytes=24 << 20),
        cost_estimate=pl.CostEstimate(
            flops=total * TILES * TILE * HEAD_WIDTH * 4,
            bytes_accessed=4 << 20,
            transcendentals=total * TILES * TILE,
        ),
        name=f"attention_{ring_step}",
    )(*operands)


def rotation(size, by):
    return [(i, (i + by) % size) for i in range(size)]


def body(
    prompt_query,
    prompt_key,
    prompt_value,
    prefix_key_cache,
    prefix_value_cache,
    decoded_query,
    decoded_key,
    decoded_value,
    shard_counts,
    block_offsets,
):
    depth = lax.axis_size("ctx_1")
    x, z, core = (lax.axis_index(a) for a in CTX)
    where = jnp.stack([x, z, core]).astype(jnp.int32)
    offsets = block_offsets.reshape(-1)
    counts = shard_counts.reshape(-1)

    def key_value_of(head):
        keys = jnp.concatenate([prompt_key, prefix_key_cache], 0)
        values = jnp.concatenate([prompt_value, prefix_value_cache], 0)
        at = head * HEAD_WIDTH
        return jnp.concatenate(
            [
                lax.dynamic_slice_in_dim(keys, at, HEAD_WIDTH, 1),
                lax.dynamic_slice_in_dim(values, at, HEAD_WIDTH, 1),
            ],
            1,
        )

    def heads_at(by):
        return lax.rem(x + by, COLUMNS)

    parts = [key_value_of(x)]
    for by in range(1, COLUMNS):
        parts.append(lax.ppermute(key_value_of(heads_at(by)), "ctx_0", rotation(COLUMNS, by)))

    def query_of(head):
        return lax.dynamic_slice_in_dim(prompt_query, head * GROUP_WIDTH, GROUP_WIDTH, 1)

    queries = [query_of(x)]
    for by in range(1, COLUMNS):
        queries.append(lax.ppermute(query_of(heads_at(by)), "ctx_0", rotation(COLUMNS, by)))

    own = jnp.concatenate(
        [p[:HALF] for p in parts] + [p[2 * HALF :] for p in parts] + [p[HALF : 2 * HALF] for p in parts],
        0,
    )
    query = jnp.stack(queries)

    def to_rows(vector, rows):
        part = lax.dynamic_slice_in_dim(vector.reshape(COLUMNS, -1), x, 1, 0)
        part = part.reshape(-1, HEAD_WIDTH)
        return jnp.concatenate([part, jnp.zeros((rows - part.shape[0], HEAD_WIDTH), part.dtype)], 0)

    decode_query = to_rows(decoded_query, 16)
    decode_key = lax.dynamic_slice_in_dim(decoded_key.reshape(COLUMNS, HEAD_WIDTH), x, 1, 0)
    decode_value = lax.dynamic_slice_in_dim(decoded_value.reshape(COLUMNS, HEAD_WIDTH), x, 1, 0)
    decode = [decode_query, decode_key, decode_value]

    ring = []
    for i in range(depth):
        ring.append((i * CORES, ((i + 1) % depth) * CORES))
        ring.append((i * CORES + 1, ((i - 1) % depth) * CORES + 1))

    def pass_on(block):
        return lax.ppermute(block, RING, ring)

    def swap(block):
        return lax.ppermute(block, "ctx_2", rotation(CORES, 1))

    step = functools.partial(run_step, where, offsets, counts, depth=depth, query=query, decode=decode)
    first, second = own, swap(own)
    state = step(
        blocks=[first, second],
        flips=((False, False), (False, True)),
        ring_step=0,
        state=None,
        last=False,
    )
    for s in range(1, depth // 2):
        first, second = pass_on(first), pass_on(second)
        state = step(
            blocks=[first, second, swap(first), swap(second)],
            flips=((False, False), (False, True), (True, True), (True, False)),
            ring_step=s,
            state=state,
            last=False,
        )
    first = pass_on(first)
    out = step(
        blocks=[first, swap(first)],
        flips=((False, False), (True, True)),
        ring_step=depth // 2,
        state=state,
        last=True,
    )

    back = [out[0]]
    for by in range(1, COLUMNS):
        back.append(lax.ppermute(out[by], "ctx_0", rotation(COLUMNS, -by)))
    joined = jnp.concatenate(back + back[:-1], 1)
    joined = lax.dynamic_slice_in_dim(
        joined, lax.rem(COLUMNS - x, COLUMNS) * GROUP_WIDTH, COLUMNS * GROUP_WIDTH, 1
    )
    return joined[: 2 * HALF], joined[2 * HALF]


def solution(mesh):
    groups = mesh.shape["groups"]
    split = Mesh(
        mesh.devices.reshape(groups, COLUMNS, -1, CORES), ("groups", *CTX)
    )
    return jax.shard_map(
        body,
        mesh=split,
        in_specs=(
            P(GROUPS_CTX, None),
            P(GROUPS_CTX, None),
            P(GROUPS_CTX, None),
            P(GROUPS_CTX, None),
            P(GROUPS_CTX, None),
            P("groups"),
            P("groups"),
            P("groups"),
            P("groups", None),
            P("groups", None),
        ),
        out_specs=(P(GROUPS_CTX, None), P("groups")),
        check_vma=False,
    )
```

```python
import functools

import jax
import jax.numpy as jnp
from jax import lax
from jax.experimental import pallas as pl
from jax.experimental.pallas import tpu as pltpu
from jax.sharding import Mesh
from jax.sharding import PartitionSpec as P

KEY_VALUE_HEADS = 4
HEAD_WIDTH = 128
HEADS_PER_GROUP = 8
GROUP_WIDTH = HEADS_PER_GROUP * HEAD_WIDTH
CTX = ("ctx_0", "ctx_1", "ctx_2")
GROUPS_CTX = ("groups", "ctx_0", "ctx_1", "ctx_2")
RING = ("ctx_1", "ctx_2")
COLUMNS = KEY_VALUE_HEADS
CORES = 2
HALF = 32
PREFIX = 8
LOW = COLUMNS * HALF
NEAR = LOW + COLUMNS * PREFIX
BLOCK = NEAR + LOW
TILES = 2 * COLUMNS
TILE = HALF * HEADS_PER_GROUP
NEGATIVE_FILL = -1e30
EXP2_SCALE = HEAD_WIDTH**-0.5 * 1.4426950408889634
NT = (((1,), (1,)), ((), ()))


def source_index(where_ref, column, ring_step, flip, depth):
    x, z, core = where_ref[0], where_ref[1], where_ref[2]
    way = jnp.where(core == 0, -ring_step, ring_step)
    if flip[0]:
        way = -way
    z_from = lax.rem(z + way + depth, depth)
    core_from = 1 - core if flip[1] else core
    x_from = lax.rem(x - column + COLUMNS, COLUMNS)
    return (x_from * depth + z_from) * CORES + core_from


def attention_step(
    where_ref, offset_ref, count_ref, *refs, flips, depth, first, last
):
    blocks = refs[: len(flips)]
    refs = refs[len(flips) :]
    query_ref, decode_query_ref = refs[:2]
    refs = refs[2:]
    if last:
        decode_key_ref, decode_value_ref = refs[:2]
        refs = refs[2:]
    if not first:
        acc_in, stats_in, decode_in = refs[:3]
        refs = refs[3:]
    if last:
        out_ref = refs[0]
        refs = refs[1:]
    else:
        acc_out, stats_out, decode_out = refs[:3]
        refs = refs[3:]
    keys, values_t, *tiles, pending = refs
    score_refs, weight_refs, peak_refs = tiles[:2], tiles[2:4], tiles[4:]

    count = len(flips)
    near, total = count * NEAR, count * BLOCK
    for b, block in enumerate(blocks):
        keys[b * NEAR : (b + 1) * NEAR, :] = block[:NEAR, :HEAD_WIDTH]
        keys[near + b * LOW : near + (b + 1) * LOW, :] = block[NEAR:, :HEAD_WIDTH]
    values = jnp.concatenate(
        [block[:NEAR, HEAD_WIDTH:] for block in blocks]
        + [block[NEAR:, HEAD_WIDTH:] for block in blocks],
        0,
    )
    values_t[...] = values.T

    ring_step = where_ref[3]
    sources = [
        [source_index(where_ref, j, ring_step, flip, depth) for j in range(COLUMNS)]
        for flip in flips
    ]
    bounds = (near, total)
    if first:
        spread = lax.broadcasted_iota(jnp.int32, (HALF, TILE), 0) - lax.rem(
            lax.broadcasted_iota(jnp.int32, (HALF, TILE), 1), HALF
        )

    def pieces(column, half):
        own = source_index(where_ref, column, 0, (False, False), depth)
        base = offset_ref[own * 2 + half]
        found = []
        for b in range(count):
            at = b * NEAR
            for j in range(COLUMNS):
                gap = None if half else base - offset_ref[sources[b][j] * 2]
                found.append((at + j * HALF, HALF, gap))
            found.append((at + LOW, NEAR - LOW, None))
        if half:
            for b in range(count):
                for j in range(COLUMNS):
                    gap = base - offset_ref[sources[b][j] * 2 + 1]
                    found.append((near + b * LOW + j * HALF, HALF, gap))
        return found

    def score(column, half):
        rows = bounds[half]
        query = jnp.concatenate(
            [
                query_ref[column, half * HALF : (half + 1) * HALF, h * HEAD_WIDTH : (h + 1) * HEAD_WIDTH]
                for h in range(HEADS_PER_GROUP)
            ],
            0,
        )
        scores = lax.dot_general(keys[:rows, :], query, NT, preferred_element_type=jnp.float32)
        peak = jnp.full((8, TILE), NEGATIVE_FILL, jnp.float32)
        for at, size, gap in pieces(column, half):
            part = scores[at : at + size, :]
            if first and gap is not None:
                part = jnp.where(spread <= gap, part, NEGATIVE_FILL)
            score_refs[half][at : at + size, :] = part
            top = jnp.max(part.reshape(size // 8, 8, TILE), axis=0)
            if gap is not None and not first:
                top = jnp.where(gap > 0, top, NEGATIVE_FILL)
            peak = jnp.maximum(peak, top)
        peak_refs[half][...] = peak

    def weigh(column, half):
        tile = column * 2 + half
        peak = jnp.max(peak_refs[half][...], axis=0, keepdims=True)
        if not first:
            old_peak = stats_in[tile, 0:1, :]
            peak = jnp.maximum(peak, old_peak)
        peak8 = jnp.broadcast_to(peak, (8, TILE))
        totals = jnp.zeros((8, TILE), jnp.float32)
        for at, size, gap in pieces(column, half):
            level = peak8
            if gap is not None and not first:
                level = jnp.where(gap > 0, peak8, -NEGATIVE_FILL)
            part = score_refs[half][at : at + size, :].reshape(size // 8, 8, TILE)
            weights = jnp.exp2((part - level[None]) * EXP2_SCALE)
            totals = totals + jnp.sum(weights, axis=0)
            weight_refs[half][at : at + size, :] = weights.reshape(size, TILE).astype(jnp.bfloat16)
        totals = jnp.sum(totals, axis=0, keepdims=True)
        if not first:
            rescale = jnp.exp2((old_peak - peak) * EXP2_SCALE)
            totals = totals + rescale * stats_in[tile, 1:2, :]
            pending[half, 0:1, :] = rescale
        if last:
            pending[half, 1:2, :] = totals
        else:
            stats_out[tile, 0:1, :] = peak
            stats_out[tile, 1:2, :] = totals

    def mix(column, half, tile):
        rows = bounds[half]
        mixture = jnp.dot(
            values_t[:, :rows], weight_refs[half][...], preferred_element_type=jnp.float32
        )
        if not first:
            mixture = mixture + pending[half, 0:1, :] * acc_in[tile]
        if last:
            own = source_index(where_ref, column, 0, (False, False), depth)
            live = count_ref[own * 2 + half]
            slot = lax.rem(lax.broadcasted_iota(jnp.int32, (1, TILE), 1), HALF)
            factor = jnp.where(slot < live, 1.0 / pending[half, 1:2, :], 0.0)
            result = (mixture * factor).T.astype(jnp.bfloat16)
            for h in range(HEADS_PER_GROUP):
                out_ref[column, half * HALF : (half + 1) * HALF, h * HEAD_WIDTH : (h + 1) * HEAD_WIDTH] = (
                    result[h * HALF : (h + 1) * HALF, :]
                )
        else:
            acc_out[tile] = mixture

    score(0, 0)

    def column_step(column, carry):
        before = jnp.maximum(column - 1, 0)
        mix(before, 1, jnp.where(column == 0, TILES, before * 2 + 1))
        score(column, 1)
        weigh(column, 0)
        mix(column, 0, column * 2)
        score(jnp.minimum(column + 1, COLUMNS - 1), 0)
        weigh(column, 1)
        return carry

    lax.fori_loop(0, COLUMNS, column_step, 0)
    mix(COLUMNS - 1, 1, TILES - 1)

    scores = lax.dot_general(
        decode_query_ref[...], keys[...], NT, preferred_element_type=jnp.float32
    )
    lane = lax.broadcasted_iota(jnp.int32, (1, total), 1)
    live = jnp.full((1, total), HALF, jnp.int32)
    for b in range(count):
        for j in range(COLUMNS):
            at = near + b * LOW + j * HALF
            live = jnp.where(
                (lane >= at) & (lane < at + HALF), count_ref[sources[b][j] * 2 + 1], live
            )
    scores = jnp.where(lax.rem(lane, HALF) < live, scores, NEGATIVE_FILL)
    peak = jnp.max(scores, axis=1, keepdims=True)
    if not first:
        old_peak = decode_in[:, HEAD_WIDTH : HEAD_WIDTH + 1]
        peak = jnp.maximum(peak, old_peak)
    weights = jnp.exp2((scores - peak) * EXP2_SCALE)
    totals = jnp.sum(weights, axis=1, keepdims=True)
    mixture = lax.dot_general(
        weights.astype(jnp.bfloat16), values_t[...], NT, preferred_element_type=jnp.float32
    )
    if not first:
        rescale = jnp.exp2((old_peak - peak) * EXP2_SCALE)
        totals = totals + rescale * decode_in[:, 2 * HEAD_WIDTH : 2 * HEAD_WIDTH + 1]
        mixture = mixture + rescale * decode_in[:, :HEAD_WIDTH]
    if last:
        query = decode_query_ref[...].astype(jnp.float32)
        own_score = jnp.sum(
            query * decode_key_ref[...].astype(jnp.float32), axis=1, keepdims=True
        )
        top = jnp.maximum(peak, own_score)
        keep = jnp.exp2((peak - top) * EXP2_SCALE)
        own_weight = jnp.exp2((own_score - top) * EXP2_SCALE)
        numerator = keep * mixture + own_weight * decode_value_ref[...].astype(jnp.float32)
        result = numerator / (keep * totals + own_weight)
        for column in range(COLUMNS):
            for h in range(HEADS_PER_GROUP):
                out_ref[column, 2 * HALF : 2 * HALF + 8, h * HEAD_WIDTH : (h + 1) * HEAD_WIDTH] = (
                    jnp.broadcast_to(result[h : h + 1, :], (8, HEAD_WIDTH)).astype(jnp.bfloat16)
                )
    else:
        decode_out[:, :HEAD_WIDTH] = mixture
        decode_out[:, HEAD_WIDTH : 2 * HEAD_WIDTH] = jnp.broadcast_to(peak, mixture.shape)
        decode_out[:, 2 * HEAD_WIDTH :] = jnp.broadcast_to(totals, mixture.shape)


STATE = (
    jax.ShapeDtypeStruct((TILES + 1, HEAD_WIDTH, TILE), jnp.float32),
    jax.ShapeDtypeStruct((TILES, 8, TILE), jnp.float32),
    jax.ShapeDtypeStruct((16, 3 * HEAD_WIDTH), jnp.float32),
)


def run_step(offsets, counts, where, blocks, flips, depth, query, decode, state, last):
    first = state is None
    smem = pl.BlockSpec(memory_space=pltpu.SMEM)
    vmem = pl.BlockSpec(memory_space=pltpu.VMEM)
    operands = [where, offsets, counts, *blocks, query, decode[0]]
    if last:
        operands += decode[1:]
    aliases = {}
    if not first:
        if not last:
            aliases = {len(operands) + i: i for i in range(3)}
        operands += state
    near, total = len(blocks) * NEAR, len(blocks) * BLOCK
    if last:
        out_shape = jax.ShapeDtypeStruct((COLUMNS, 2 * HALF + 8, GROUP_WIDTH), jnp.bfloat16)
        out_specs = vmem
    else:
        out_shape, out_specs = STATE, (vmem,) * 3
    kernel = functools.partial(
        attention_step, flips=flips, depth=depth, first=first, last=last
    )
    return pl.pallas_call(
        kernel,
        out_shape=out_shape,
        in_specs=[smem] * 3 + [vmem] * (len(operands) - 3),
        out_specs=out_specs,
        scratch_shapes=[
            pltpu.VMEM((total, HEAD_WIDTH), jnp.bfloat16),
            pltpu.VMEM((HEAD_WIDTH, total), jnp.bfloat16),
            pltpu.VMEM((near, TILE), jnp.float32),
            pltpu.VMEM((total, TILE), jnp.float32),
            pltpu.VMEM((near, TILE), jnp.bfloat16),
            pltpu.VMEM((total, TILE), jnp.bfloat16),
            pltpu.VMEM((8, TILE), jnp.float32),
            pltpu.VMEM((8, TILE), jnp.float32),
            pltpu.VMEM((2, 8, TILE), jnp.float32),
        ],
        input_output_aliases=aliases,
        compiler_params=pltpu.CompilerParams(vmem_limit_bytes=24 << 20),
        cost_estimate=pl.CostEstimate(
            flops=total * TILES * TILE * HEAD_WIDTH * 4,
            bytes_accessed=4 << 20,
            transcendentals=total * TILES * TILE,
        ),
        name="attention_first" if first else "attention_last" if last else "attention",
    )(*operands)


def rotation(size, by):
    return [(i, (i + by) % size) for i in range(size)]


def body(
    prompt_query,
    prompt_key,
    prompt_value,
    prefix_key_cache,
    prefix_value_cache,
    decoded_query,
    decoded_key,
    decoded_value,
    shard_counts,
    block_offsets,
):
    depth = lax.axis_size("ctx_1")
    x, z, core = (lax.axis_index(a) for a in CTX)
    where = jnp.stack([x, z, core, jnp.zeros_like(x)]).astype(jnp.int32)
    offsets = block_offsets.reshape(-1)
    counts = shard_counts.reshape(-1)

    def key_value_of(head):
        keys = jnp.concatenate([prompt_key, prefix_key_cache], 0)
        values = jnp.concatenate([prompt_value, prefix_value_cache], 0)
        at = head * HEAD_WIDTH
        return jnp.concatenate(
            [
                lax.dynamic_slice_in_dim(keys, at, HEAD_WIDTH, 1),
                lax.dynamic_slice_in_dim(values, at, HEAD_WIDTH, 1),
            ],
            1,
        )

    def heads_at(by):
        return lax.rem(x + by, COLUMNS)

    parts = [key_value_of(x)]
    for by in range(1, COLUMNS):
        parts.append(lax.ppermute(key_value_of(heads_at(by)), "ctx_0", rotation(COLUMNS, by)))

    def query_of(head):
        return lax.dynamic_slice_in_dim(prompt_query, head * GROUP_WIDTH, GROUP_WIDTH, 1)

    queries = [query_of(x)]
    for by in range(1, COLUMNS):
        mine = query_of(heads_at(by))
        queries.append(lax.ppermute(mine, "ctx_0", rotation(COLUMNS, by)))

    own = jnp.concatenate(
        [p[:HALF] for p in parts] + [p[2 * HALF :] for p in parts] + [p[HALF : 2 * HALF] for p in parts],
        0,
    )
    query = jnp.stack(queries)

    def to_rows(vector, rows):
        part = lax.dynamic_slice_in_dim(vector.reshape(COLUMNS, -1), x, 1, 0)
        part = part.reshape(-1, HEAD_WIDTH)
        return jnp.concatenate([part, jnp.zeros((rows - part.shape[0], HEAD_WIDTH), part.dtype)], 0)

    decode_query = to_rows(decoded_query, 16)
    decode_key = lax.dynamic_slice_in_dim(decoded_key.reshape(COLUMNS, HEAD_WIDTH), x, 1, 0)
    decode_value = lax.dynamic_slice_in_dim(decoded_value.reshape(COLUMNS, HEAD_WIDTH), x, 1, 0)
    decode = [decode_query, decode_key, decode_value]

    ring = []
    for i in range(depth):
        ring.append((i * CORES, ((i + 1) % depth) * CORES))
        ring.append((i * CORES + 1, ((i - 1) % depth) * CORES + 1))

    def pass_on(block):
        return lax.ppermute(block, RING, ring)

    def swap(block):
        return lax.ppermute(block, "ctx_2", rotation(CORES, 1))

    step = functools.partial(run_step, offsets, counts, depth=depth, query=query, decode=decode)
    near_flips = ((False, False), (False, True))
    far_flips = ((True, True), (True, False))
    first, second = own, swap(own)
    state = None
    for s in range(depth // 2):
        state = step(
            where=where,
            blocks=[first, second, swap(first), swap(second)] if s else [first, second],
            flips=near_flips + far_flips if s else near_flips,
            state=state,
            last=False,
        )
        first = pass_on(first)
        if s + 1 < depth // 2:
            second = pass_on(second)
        where = lax.optimization_barrier(where + jnp.array([0, 0, 0, 1], jnp.int32))
    out = step(
        where=where,
        blocks=[first, swap(first)],
        flips=((False, False), (True, True)),
        state=state,
        last=True,
    )

    back = [out[0]]
    for by in range(1, COLUMNS):
        back.append(lax.ppermute(out[by], "ctx_0", rotation(COLUMNS, -by)))
    joined = jnp.concatenate(back + back[:-1], 1)
    joined = lax.dynamic_slice_in_dim(
        joined, lax.rem(COLUMNS - x, COLUMNS) * GROUP_WIDTH, COLUMNS * GROUP_WIDTH, 1
    )
    return joined[: 2 * HALF], joined[2 * HALF]


def solution(mesh):
    groups = mesh.shape["groups"]
    split = Mesh(
        mesh.devices.reshape(groups, COLUMNS, -1, CORES), ("groups", *CTX)
    )

    return jax.shard_map(
        body,
        mesh=split,
        in_specs=(
            P(GROUPS_CTX, None),
            P(GROUPS_CTX, None),
            P(GROUPS_CTX, None),
            P(GROUPS_CTX, None),
            P(GROUPS_CTX, None),
            P("groups"),
            P("groups"),
            P("groups"),
            P("groups", None),
            P("groups", None),
        ),
        out_specs=(P(GROUPS_CTX, None), P("groups")),
        check_vma=False,
    )
```

```python
import functools

import jax
import jax.numpy as jnp
from jax import lax
from jax.experimental import pallas as pl
from jax.experimental.pallas import tpu as pltpu
from jax.sharding import Mesh
from jax.sharding import PartitionSpec as P

KEY_VALUE_HEADS = 4
HEAD_WIDTH = 128
HEADS_PER_GROUP = 8
GROUP_WIDTH = HEADS_PER_GROUP * HEAD_WIDTH
CTX = ("ctx_0", "ctx_1", "ctx_2")
GROUPS_CTX = ("groups", "ctx_0", "ctx_1", "ctx_2")
RING = ("ctx_1", "ctx_2")
COLUMNS = KEY_VALUE_HEADS
CORES = 2
HALF = 32
PREFIX = 8
LOW = COLUMNS * HALF
NEAR = LOW + COLUMNS * PREFIX
BLOCK = NEAR + LOW
TILES = 2 * COLUMNS
TILE = HALF * HEADS_PER_GROUP
NEGATIVE_FILL = -1e30
EXP2_SCALE = HEAD_WIDTH**-0.5 * 1.4426950408889634
NT = (((1,), (1,)), ((), ()))


def source_index(where_ref, column, ring_step, flip, depth):
    x, z, core = where_ref[0], where_ref[1], where_ref[2]
    way = jnp.where(core == 0, -ring_step, ring_step)
    if flip[0]:
        way = -way
    z_from = lax.rem(z + way + depth, depth)
    core_from = 1 - core if flip[1] else core
    x_from = lax.rem(x - column + COLUMNS, COLUMNS)
    return (x_from * depth + z_from) * CORES + core_from


def attention_step(
    where_ref, offset_ref, count_ref, *refs, flips, depth, first, last
):
    if len(flips) == 4:
        near_first, near_second, far = refs[:3]
        blocks = (near_first, near_second, far.at[:BLOCK], far.at[BLOCK:])
        refs = refs[3:]
    else:
        blocks, refs = refs[: len(flips)], refs[len(flips) :]
    query_ref, decode_query_ref = refs[:2]
    refs = refs[2:]
    if last:
        decode_key_ref, decode_value_ref = refs[:2]
        refs = refs[2:]
    if not first:
        acc_in, stats_in, decode_in = refs[:3]
        refs = refs[3:]
    if last:
        out_ref = refs[0]
        refs = refs[1:]
    else:
        acc_out, stats_out, decode_out = refs[:3]
        refs = refs[3:]
    keys, values_t, *tiles, pending = refs
    score_refs, weight_refs, peak_refs = tiles[:2], tiles[2:4], tiles[4:]

    count = len(flips)
    near, total = count * NEAR, count * BLOCK
    for b, block in enumerate(blocks):
        keys[b * NEAR : (b + 1) * NEAR, :] = block[:NEAR, :HEAD_WIDTH]
        keys[near + b * LOW : near + (b + 1) * LOW, :] = block[NEAR:, :HEAD_WIDTH]
    values = jnp.concatenate(
        [block[:NEAR, HEAD_WIDTH:] for block in blocks]
        + [block[NEAR:, HEAD_WIDTH:] for block in blocks],
        0,
    )
    values_t[...] = values.T

    ring_step = where_ref[3]
    sources = [
        [source_index(where_ref, j, ring_step, flip, depth) for j in range(COLUMNS)]
        for flip in flips
    ]
    bounds = (near, total)
    if first:
        spread = lax.broadcasted_iota(jnp.int32, (HALF, TILE), 0) - lax.rem(
            lax.broadcasted_iota(jnp.int32, (HALF, TILE), 1), HALF
        )

    def pieces(column, half):
        own = source_index(where_ref, column, 0, (False, False), depth)
        base = offset_ref[own * 2 + half]
        found = []
        for b in range(count):
            at = b * NEAR
            for j in range(COLUMNS):
                gap = None if half else base - offset_ref[sources[b][j] * 2]
                found.append((at + j * HALF, HALF, gap))
            found.append((at + LOW, NEAR - LOW, None))
        if half:
            for b in range(count):
                for j in range(COLUMNS):
                    gap = base - offset_ref[sources[b][j] * 2 + 1]
                    found.append((near + b * LOW + j * HALF, HALF, gap))
        return found

    def score(column, half):
        rows = bounds[half]
        query = jnp.concatenate(
            [
                query_ref[column, half * HALF : (half + 1) * HALF, h * HEAD_WIDTH : (h + 1) * HEAD_WIDTH]
                for h in range(HEADS_PER_GROUP)
            ],
            0,
        )
        scores = lax.dot_general(keys[:rows, :], query, NT, preferred_element_type=jnp.float32)
        peak = jnp.full((8, TILE), NEGATIVE_FILL, jnp.float32)
        for at, size, gap in pieces(column, half):
            part = scores[at : at + size, :]
            if first and gap is not None:
                part = jnp.where(spread <= gap, part, NEGATIVE_FILL)
            score_refs[half][at : at + size, :] = part
            top = jnp.max(part.reshape(size // 8, 8, TILE), axis=0)
            if gap is not None and not first:
                top = jnp.where(gap > 0, top, NEGATIVE_FILL)
            peak = jnp.maximum(peak, top)
        peak_refs[half][...] = peak

    def weigh(column, half):
        tile = column * 2 + half
        peak = jnp.max(peak_refs[half][...], axis=0, keepdims=True)
        if not first:
            old_peak = stats_in[tile, 0:1, :]
            peak = jnp.maximum(peak, old_peak)
        peak8 = jnp.broadcast_to(peak, (8, TILE))
        totals = jnp.zeros((8, TILE), jnp.float32)
        for at, size, gap in pieces(column, half):
            level = peak8
            if gap is not None and not first:
                level = jnp.where(gap > 0, peak8, -NEGATIVE_FILL)
            part = score_refs[half][at : at + size, :].reshape(size // 8, 8, TILE)
            weights = jnp.exp2((part - level[None]) * EXP2_SCALE)
            totals = totals + jnp.sum(weights, axis=0)
            weight_refs[half][at : at + size, :] = weights.reshape(size, TILE).astype(jnp.bfloat16)
        totals = jnp.sum(totals, axis=0, keepdims=True)
        if not first:
            rescale = jnp.exp2((old_peak - peak) * EXP2_SCALE)
            totals = totals + rescale * stats_in[tile, 1:2, :]
            pending[half, 0:1, :] = rescale
        if last:
            pending[half, 1:2, :] = totals
        else:
            stats_out[tile, 0:1, :] = peak
            stats_out[tile, 1:2, :] = totals

    def mix(column, half, tile):
        rows = bounds[half]
        mixture = jnp.dot(
            values_t[:, :rows], weight_refs[half][...], preferred_element_type=jnp.float32
        )
        if not first:
            mixture = mixture + pending[half, 0:1, :] * acc_in[tile]
        if last:
            own = source_index(where_ref, column, 0, (False, False), depth)
            live = count_ref[own * 2 + half]
            slot = lax.rem(lax.broadcasted_iota(jnp.int32, (1, TILE), 1), HALF)
            factor = jnp.where(slot < live, 1.0 / pending[half, 1:2, :], 0.0)
            result = (mixture * factor).T.astype(jnp.bfloat16)
            for h in range(HEADS_PER_GROUP):
                out_ref[column, half * HALF : (half + 1) * HALF, h * HEAD_WIDTH : (h + 1) * HEAD_WIDTH] = (
                    result[h * HALF : (h + 1) * HALF, :]
                )
        else:
            acc_out[tile] = mixture

    score(0, 0)

    def column_step(column, carry):
        before = jnp.maximum(column - 1, 0)
        mix(before, 1, jnp.where(column == 0, TILES, before * 2 + 1))
        score(column, 1)
        weigh(column, 0)
        mix(column, 0, column * 2)
        score(jnp.minimum(column + 1, COLUMNS - 1), 0)
        weigh(column, 1)
        return carry

    lax.fori_loop(0, COLUMNS, column_step, 0)
    mix(COLUMNS - 1, 1, TILES - 1)

    scores = lax.dot_general(
        decode_query_ref[...], keys[...], NT, preferred_element_type=jnp.float32
    )
    lane = lax.broadcasted_iota(jnp.int32, (1, total), 1)
    live = jnp.full((1, total), HALF, jnp.int32)
    for b in range(count):
        for j in range(COLUMNS):
            at = near + b * LOW + j * HALF
            live = jnp.where(
                (lane >= at) & (lane < at + HALF), count_ref[sources[b][j] * 2 + 1], live
            )
    scores = jnp.where(lax.rem(lane, HALF) < live, scores, NEGATIVE_FILL)
    peak = jnp.max(scores, axis=1, keepdims=True)
    if not first:
        old_peak = decode_in[:, HEAD_WIDTH : HEAD_WIDTH + 1]
        peak = jnp.maximum(peak, old_peak)
    weights = jnp.exp2((scores - peak) * EXP2_SCALE)
    totals = jnp.sum(weights, axis=1, keepdims=True)
    mixture = lax.dot_general(
        weights.astype(jnp.bfloat16), values_t[...], NT, preferred_element_type=jnp.float32
    )
    if not first:
        rescale = jnp.exp2((old_peak - peak) * EXP2_SCALE)
        totals = totals + rescale * decode_in[:, 2 * HEAD_WIDTH : 2 * HEAD_WIDTH + 1]
        mixture = mixture + rescale * decode_in[:, :HEAD_WIDTH]
    if last:
        query = decode_query_ref[...].astype(jnp.float32)
        own_score = jnp.sum(
            query * decode_key_ref[...].astype(jnp.float32), axis=1, keepdims=True
        )
        top = jnp.maximum(peak, own_score)
        keep = jnp.exp2((peak - top) * EXP2_SCALE)
        own_weight = jnp.exp2((own_score - top) * EXP2_SCALE)
        numerator = keep * mixture + own_weight * decode_value_ref[...].astype(jnp.float32)
        result = numerator / (keep * totals + own_weight)
        for column in range(COLUMNS):
            for h in range(HEADS_PER_GROUP):
                out_ref[column, 2 * HALF : 2 * HALF + 8, h * HEAD_WIDTH : (h + 1) * HEAD_WIDTH] = (
                    jnp.broadcast_to(result[h : h + 1, :], (8, HEAD_WIDTH)).astype(jnp.bfloat16)
                )
    else:
        decode_out[:, :HEAD_WIDTH] = mixture
        decode_out[:, HEAD_WIDTH : 2 * HEAD_WIDTH] = jnp.broadcast_to(peak, mixture.shape)
        decode_out[:, 2 * HEAD_WIDTH :] = jnp.broadcast_to(totals, mixture.shape)


STATE = (
    jax.ShapeDtypeStruct((TILES + 1, HEAD_WIDTH, TILE), jnp.float32),
    jax.ShapeDtypeStruct((TILES, 8, TILE), jnp.float32),
    jax.ShapeDtypeStruct((16, 3 * HEAD_WIDTH), jnp.float32),
)


def run_step(offsets, counts, where, blocks, flips, depth, query, decode, state, last):
    first = state is None
    smem = pl.BlockSpec(memory_space=pltpu.SMEM)
    vmem = pl.BlockSpec(memory_space=pltpu.VMEM)
    operands = [where, offsets, counts, *blocks, query, decode[0]]
    if last:
        operands += decode[1:]
    aliases = {}
    if not first:
        if not last:
            aliases = {len(operands) + i: i for i in range(3)}
        operands += state
    near, total = len(flips) * NEAR, len(flips) * BLOCK
    if last:
        out_shape = jax.ShapeDtypeStruct((COLUMNS, 2 * HALF + 8, GROUP_WIDTH), jnp.bfloat16)
        out_specs = vmem
    else:
        out_shape, out_specs = STATE, (vmem,) * 3
    kernel = functools.partial(
        attention_step, flips=flips, depth=depth, first=first, last=last
    )
    return pl.pallas_call(
        kernel,
        out_shape=out_shape,
        in_specs=[smem] * 3 + [vmem] * (len(operands) - 3),
        out_specs=out_specs,
        scratch_shapes=[
            pltpu.VMEM((total, HEAD_WIDTH), jnp.bfloat16),
            pltpu.VMEM((HEAD_WIDTH, total), jnp.bfloat16),
            pltpu.VMEM((near, TILE), jnp.float32),
            pltpu.VMEM((total, TILE), jnp.float32),
            pltpu.VMEM((near, TILE), jnp.bfloat16),
            pltpu.VMEM((total, TILE), jnp.bfloat16),
            pltpu.VMEM((8, TILE), jnp.float32),
            pltpu.VMEM((8, TILE), jnp.float32),
            pltpu.VMEM((2, 8, TILE), jnp.float32),
        ],
        input_output_aliases=aliases,
        compiler_params=pltpu.CompilerParams(vmem_limit_bytes=12 << 20),
        cost_estimate=pl.CostEstimate(
            flops=total * TILES * TILE * HEAD_WIDTH * 4,
            bytes_accessed=4 << 20,
            transcendentals=total * TILES * TILE,
        ),
        name="attention_first" if first else "attention_last" if last else "attention",
    )(*operands)


def rotation(size, by):
    return [(i, (i + by) % size) for i in range(size)]


def body(
    prompt_query,
    prompt_key,
    prompt_value,
    prefix_key_cache,
    prefix_value_cache,
    decoded_query,
    decoded_key,
    decoded_value,
    shard_counts,
    block_offsets,
):
    depth = lax.axis_size("ctx_1")
    x, z, core = (lax.axis_index(a) for a in CTX)
    where = jnp.stack([x, z, core, jnp.zeros_like(x)]).astype(jnp.int32)
    offsets = block_offsets.reshape(-1)
    counts = shard_counts.reshape(-1)

    def key_value_of(head):
        keys = jnp.concatenate([prompt_key, prefix_key_cache], 0)
        values = jnp.concatenate([prompt_value, prefix_value_cache], 0)
        at = head * HEAD_WIDTH
        return jnp.concatenate(
            [
                lax.dynamic_slice_in_dim(keys, at, HEAD_WIDTH, 1),
                lax.dynamic_slice_in_dim(values, at, HEAD_WIDTH, 1),
            ],
            1,
        )

    def heads_at(by):
        return lax.rem(x + by, COLUMNS)

    parts = [key_value_of(x)]
    for by in range(1, COLUMNS):
        parts.append(lax.ppermute(key_value_of(heads_at(by)), "ctx_0", rotation(COLUMNS, by)))

    def query_of(head):
        return lax.dynamic_slice_in_dim(prompt_query, head * GROUP_WIDTH, GROUP_WIDTH, 1)

    queries = [query_of(x)]
    for by in range(1, COLUMNS):
        mine = query_of(heads_at(by))
        queries.append(lax.ppermute(mine, "ctx_0", rotation(COLUMNS, by)))

    own = jnp.concatenate(
        [p[:HALF] for p in parts] + [p[2 * HALF :] for p in parts] + [p[HALF : 2 * HALF] for p in parts],
        0,
    )
    query = jnp.stack(queries)

    def to_rows(vector, rows):
        part = lax.dynamic_slice_in_dim(vector.reshape(COLUMNS, -1), x, 1, 0)
        part = part.reshape(-1, HEAD_WIDTH)
        return jnp.concatenate([part, jnp.zeros((rows - part.shape[0], HEAD_WIDTH), part.dtype)], 0)

    decode_query = to_rows(decoded_query, 16)
    decode_key = lax.dynamic_slice_in_dim(decoded_key.reshape(COLUMNS, HEAD_WIDTH), x, 1, 0)
    decode_value = lax.dynamic_slice_in_dim(decoded_value.reshape(COLUMNS, HEAD_WIDTH), x, 1, 0)
    decode = [decode_query, decode_key, decode_value]

    ring = []
    for i in range(depth):
        ring.append((i * CORES, ((i + 1) % depth) * CORES))
        ring.append((i * CORES + 1, ((i - 1) % depth) * CORES + 1))

    def pass_on(block):
        return lax.ppermute(block, RING, ring)

    def swap(block):
        return lax.ppermute(block, "ctx_2", rotation(CORES, 1))

    step = functools.partial(run_step, offsets, counts, depth=depth, query=query, decode=decode)
    near_flips = ((False, False), (False, True))
    far_flips = ((True, True), (True, False))
    first, second = own, swap(own)
    state = None
    for s in range(depth // 2):
        blocks = [first, second]
        if s:
            blocks.append(swap(jnp.concatenate([first, second], 0)))
        state = step(
            where=where,
            blocks=blocks,
            flips=near_flips + far_flips if s else near_flips,
            state=state,
            last=False,
        )
        first = pass_on(first)
        if s + 1 < depth // 2:
            second = pass_on(second)
        where = lax.optimization_barrier(where + jnp.array([0, 0, 0, 1], jnp.int32))
    out = step(
        where=where,
        blocks=[first, swap(first)],
        flips=((False, False), (True, True)),
        state=state,
        last=True,
    )

    back = [out[0]]
    for by in range(1, COLUMNS):
        back.append(lax.ppermute(out[by], "ctx_0", rotation(COLUMNS, -by)))
    joined = jnp.concatenate(back + back[:-1], 1)
    joined = lax.dynamic_slice_in_dim(
        joined, lax.rem(COLUMNS - x, COLUMNS) * GROUP_WIDTH, COLUMNS * GROUP_WIDTH, 1
    )
    return joined[: 2 * HALF], joined[2 * HALF]


def solution(mesh):
    groups = mesh.shape["groups"]
    split = Mesh(
        mesh.devices.reshape(groups, COLUMNS, -1, CORES), ("groups", *CTX)
    )

    return jax.shard_map(
        body,
        mesh=split,
        in_specs=(
            P(GROUPS_CTX, None),
            P(GROUPS_CTX, None),
            P(GROUPS_CTX, None),
            P(GROUPS_CTX, None),
            P(GROUPS_CTX, None),
            P("groups"),
            P("groups"),
            P("groups"),
            P("groups", None),
            P("groups", None),
        ),
        out_specs=(P(GROUPS_CTX, None), P("groups")),
        check_vma=False,
    )
```

```python
import functools

import jax
import jax.numpy as jnp
from jax import lax
from jax.experimental import pallas as pl
from jax.experimental.pallas import tpu as pltpu
from jax.sharding import Mesh
from jax.sharding import PartitionSpec as P

KEY_VALUE_HEADS = 4
HEAD_WIDTH = 128
HEADS_PER_GROUP = 8
GROUP_WIDTH = HEADS_PER_GROUP * HEAD_WIDTH
CTX = ("ctx_0", "ctx_1", "ctx_2")
GROUPS_CTX = ("groups", "ctx_0", "ctx_1", "ctx_2")
RING = ("ctx_1", "ctx_2")
COLUMNS = KEY_VALUE_HEADS
CORES = 2
HALF = 32
PREFIX = 8
LOW = COLUMNS * HALF
NEAR = LOW + COLUMNS * PREFIX
BLOCK = NEAR + LOW
TILES = 2 * COLUMNS
TILE = HALF * HEADS_PER_GROUP
NEGATIVE_FILL = -1e30
EXP2_SCALE = HEAD_WIDTH**-0.5 * 1.4426950408889634
NT = (((1,), (1,)), ((), ()))


def source_index(where_ref, column, ring_step, flip, depth):
    x, z, core = where_ref[0], where_ref[1], where_ref[2]
    way = jnp.where(core == 0, -ring_step, ring_step)
    if flip[0]:
        way = -way
    z_from = lax.rem(z + way + depth, depth)
    core_from = 1 - core if flip[1] else core
    x_from = lax.rem(x - column + COLUMNS, COLUMNS)
    return (x_from * depth + z_from) * CORES + core_from


def attention_step(
    where_ref, offset_ref, count_ref, *refs, flips, depth, first, last
):
    if len(flips) == 4:
        near_first, near_second, far = refs[:3]
        blocks = (near_first, near_second, far.at[:BLOCK], far.at[BLOCK:])
        refs = refs[3:]
    else:
        blocks, refs = refs[: len(flips)], refs[len(flips) :]
    query_ref, decode_query_ref = refs[:2]
    refs = refs[2:]
    if last:
        decode_key_ref, decode_value_ref = refs[:2]
        refs = refs[2:]
    if not first:
        acc_in, stats_in, decode_in = refs[:3]
        refs = refs[3:]
    if last:
        out_ref = refs[0]
        refs = refs[1:]
    else:
        acc_out, stats_out, decode_out = refs[:3]
        refs = refs[3:]
    keys, values_t, *tiles, pending = refs
    score_refs, weight_refs, peak_refs = tiles[:2], tiles[2:4], tiles[4:]

    count = len(flips)
    near, total = count * NEAR, count * BLOCK
    for b, block in enumerate(blocks):
        keys[b * NEAR : (b + 1) * NEAR, :] = block[:NEAR, :HEAD_WIDTH]
        keys[near + b * LOW : near + (b + 1) * LOW, :] = block[NEAR:, :HEAD_WIDTH]
    values = jnp.concatenate(
        [block[:NEAR, HEAD_WIDTH:] for block in blocks]
        + [block[NEAR:, HEAD_WIDTH:] for block in blocks],
        0,
    )
    values_t[...] = values.T

    ring_step = where_ref[3]
    sources = [
        [source_index(where_ref, j, ring_step, flip, depth) for j in range(COLUMNS)]
        for flip in flips
    ]
    bounds = (near, total)
    if first:
        spread = lax.broadcasted_iota(jnp.int32, (HALF, TILE), 0) - lax.rem(
            lax.broadcasted_iota(jnp.int32, (HALF, TILE), 1), HALF
        )

    def pieces(column, half):
        own = source_index(where_ref, column, 0, (False, False), depth)
        base = offset_ref[own * 2 + half]
        found = []
        for b in range(count):
            at = b * NEAR
            for j in range(COLUMNS):
                gap = None if half else base - offset_ref[sources[b][j] * 2]
                found.append((at + j * HALF, HALF, gap))
            found.append((at + LOW, NEAR - LOW, None))
        if half:
            for b in range(count):
                for j in range(COLUMNS):
                    gap = base - offset_ref[sources[b][j] * 2 + 1]
                    found.append((near + b * LOW + j * HALF, HALF, gap))
        return found

    def score(column, half):
        rows = bounds[half]
        query = jnp.concatenate(
            [
                query_ref[column, half * HALF : (half + 1) * HALF, h * HEAD_WIDTH : (h + 1) * HEAD_WIDTH]
                for h in range(HEADS_PER_GROUP)
            ],
            0,
        )
        scores = lax.dot_general(keys[:rows, :], query, NT, preferred_element_type=jnp.float32)
        peak = jnp.full((8, TILE), NEGATIVE_FILL, jnp.float32)
        for at, size, gap in pieces(column, half):
            part = scores[at : at + size, :]
            if first and gap is not None:
                part = jnp.where(spread <= gap, part, NEGATIVE_FILL)
            score_refs[half][at : at + size, :] = part
            top = jnp.max(part.reshape(size // 8, 8, TILE), axis=0)
            if gap is not None and not first:
                top = jnp.where(gap > 0, top, NEGATIVE_FILL)
            peak = jnp.maximum(peak, top)
        peak_refs[half][...] = peak

    def weigh(column, half):
        tile = column * 2 + half
        peak = jnp.max(peak_refs[half][...], axis=0, keepdims=True)
        if not first:
            old_peak = stats_in[tile, 0:1, :]
            peak = jnp.maximum(peak, old_peak)
        peak8 = jnp.broadcast_to(peak, (8, TILE))
        totals = jnp.zeros((8, TILE), jnp.float32)
        for at, size, gap in pieces(column, half):
            level = peak8
            if gap is not None and not first:
                level = jnp.where(gap > 0, peak8, -NEGATIVE_FILL)
            part = score_refs[half][at : at + size, :].reshape(size // 8, 8, TILE)
            weights = jnp.exp2((part - level[None]) * EXP2_SCALE)
            totals = totals + jnp.sum(weights, axis=0)
            weight_refs[half][at : at + size, :] = weights.reshape(size, TILE).astype(jnp.bfloat16)
        totals = jnp.sum(totals, axis=0, keepdims=True)
        if not first:
            rescale = jnp.exp2((old_peak - peak) * EXP2_SCALE)
            totals = totals + rescale * stats_in[tile, 1:2, :]
            pending[half, 0:1, :] = rescale
        if last:
            pending[half, 1:2, :] = totals
        else:
            stats_out[tile, 0:1, :] = peak
            stats_out[tile, 1:2, :] = totals

    def mix(column, half, tile):
        rows = bounds[half]
        mixture = jnp.dot(
            values_t[:, :rows], weight_refs[half][...], preferred_element_type=jnp.float32
        )
        if not first:
            mixture = mixture + pending[half, 0:1, :] * acc_in[tile]
        if last:
            own = source_index(where_ref, column, 0, (False, False), depth)
            live = count_ref[own * 2 + half]
            slot = lax.rem(lax.broadcasted_iota(jnp.int32, (1, TILE), 1), HALF)
            factor = jnp.where(slot < live, 1.0 / pending[half, 1:2, :], 0.0)
            result = (mixture * factor).T.astype(jnp.bfloat16)
            for h in range(HEADS_PER_GROUP):
                out_ref[column, half * HALF : (half + 1) * HALF, h * HEAD_WIDTH : (h + 1) * HEAD_WIDTH] = (
                    result[h * HALF : (h + 1) * HALF, :]
                )
        else:
            acc_out[tile] = mixture

    score(0, 0)

    def column_step(column, carry):
        before = jnp.maximum(column - 1, 0)
        mix(before, 1, jnp.where(column == 0, TILES, before * 2 + 1))
        score(column, 1)
        weigh(column, 0)
        mix(column, 0, column * 2)
        score(jnp.minimum(column + 1, COLUMNS - 1), 0)
        weigh(column, 1)
        return carry

    lax.fori_loop(0, COLUMNS, column_step, 0)
    mix(COLUMNS - 1, 1, TILES - 1)

    scores = lax.dot_general(
        decode_query_ref[...], keys[...], NT, preferred_element_type=jnp.float32
    )
    lane = lax.broadcasted_iota(jnp.int32, (1, total), 1)
    live = jnp.full((1, total), HALF, jnp.int32)
    for b in range(count):
        for j in range(COLUMNS):
            at = near + b * LOW + j * HALF
            live = jnp.where(
                (lane >= at) & (lane < at + HALF), count_ref[sources[b][j] * 2 + 1], live
            )
    scores = jnp.where(lax.rem(lane, HALF) < live, scores, NEGATIVE_FILL)
    peak = jnp.max(scores, axis=1, keepdims=True)
    if not first:
        old_peak = decode_in[:, HEAD_WIDTH : HEAD_WIDTH + 1]
        peak = jnp.maximum(peak, old_peak)
    weights = jnp.exp2((scores - peak) * EXP2_SCALE)
    totals = jnp.sum(weights, axis=1, keepdims=True)
    mixture = lax.dot_general(
        weights.astype(jnp.bfloat16), values_t[...], NT, preferred_element_type=jnp.float32
    )
    if not first:
        rescale = jnp.exp2((old_peak - peak) * EXP2_SCALE)
        totals = totals + rescale * decode_in[:, 2 * HEAD_WIDTH : 2 * HEAD_WIDTH + 1]
        mixture = mixture + rescale * decode_in[:, :HEAD_WIDTH]
    if last:
        query = decode_query_ref[...].astype(jnp.float32)
        own_score = jnp.sum(
            query * decode_key_ref[...].astype(jnp.float32), axis=1, keepdims=True
        )
        top = jnp.maximum(peak, own_score)
        keep = jnp.exp2((peak - top) * EXP2_SCALE)
        own_weight = jnp.exp2((own_score - top) * EXP2_SCALE)
        numerator = keep * mixture + own_weight * decode_value_ref[...].astype(jnp.float32)
        result = numerator / (keep * totals + own_weight)
        for column in range(COLUMNS):
            out_ref[column, 2 * HALF :, :HEAD_WIDTH] = result[:HEADS_PER_GROUP, :].astype(jnp.bfloat16)
    else:
        decode_out[:, :HEAD_WIDTH] = mixture
        decode_out[:, HEAD_WIDTH : 2 * HEAD_WIDTH] = jnp.broadcast_to(peak, mixture.shape)
        decode_out[:, 2 * HEAD_WIDTH :] = jnp.broadcast_to(totals, mixture.shape)


STATE = (
    jax.ShapeDtypeStruct((TILES + 1, HEAD_WIDTH, TILE), jnp.float32),
    jax.ShapeDtypeStruct((TILES, 8, TILE), jnp.float32),
    jax.ShapeDtypeStruct((16, 3 * HEAD_WIDTH), jnp.float32),
)


def run_step(offsets, counts, where, blocks, flips, depth, query, decode, state, last):
    first = state is None
    smem = pl.BlockSpec(memory_space=pltpu.SMEM)
    vmem = pl.BlockSpec(memory_space=pltpu.VMEM)
    operands = [where, offsets, counts, *blocks, query, decode[0]]
    if last:
        operands += decode[1:]
    aliases = {}
    if not first:
        if not last:
            aliases = {len(operands) + i: i for i in range(3)}
        operands += state
    near, total = len(flips) * NEAR, len(flips) * BLOCK
    if last:
        out_shape = jax.ShapeDtypeStruct((COLUMNS, 2 * HALF + 8, GROUP_WIDTH), jnp.bfloat16)
        out_specs = vmem
    else:
        out_shape, out_specs = STATE, (vmem,) * 3
    kernel = functools.partial(
        attention_step, flips=flips, depth=depth, first=first, last=last
    )
    return pl.pallas_call(
        kernel,
        out_shape=out_shape,
        in_specs=[smem] * 3 + [vmem] * (len(operands) - 3),
        out_specs=out_specs,
        scratch_shapes=[
            pltpu.VMEM((total, HEAD_WIDTH), jnp.bfloat16),
            pltpu.VMEM((HEAD_WIDTH, total), jnp.bfloat16),
            pltpu.VMEM((near, TILE), jnp.float32),
            pltpu.VMEM((total, TILE), jnp.float32),
            pltpu.VMEM((near, TILE), jnp.bfloat16),
            pltpu.VMEM((total, TILE), jnp.bfloat16),
            pltpu.VMEM((8, TILE), jnp.float32),
            pltpu.VMEM((8, TILE), jnp.float32),
            pltpu.VMEM((2, 8, TILE), jnp.float32),
        ],
        input_output_aliases=aliases,
        compiler_params=pltpu.CompilerParams(vmem_limit_bytes=12 << 20),
        cost_estimate=pl.CostEstimate(
            flops=total * TILES * TILE * HEAD_WIDTH * 4,
            bytes_accessed=4 << 20,
            transcendentals=total * TILES * TILE,
        ),
        name="attention_first" if first else "attention_last" if last else "attention",
    )(*operands)


def place(where_ref, *refs):
    blocks, (span_ref, next_ref, semaphores) = refs[:COLUMNS], refs[COLUMNS:]
    copies = []
    for by, block in enumerate(blocks):
        head = lax.rem(where_ref[0] + by, COLUMNS)
        columns = pl.ds(pl.multiple_of(head * GROUP_WIDTH, GROUP_WIDTH), GROUP_WIDTH)
        rows = pl.ds(pl.multiple_of(head * HEADS_PER_GROUP, HEADS_PER_GROUP), HEADS_PER_GROUP)
        for source, target in (
            (block.at[: 2 * HALF, :], span_ref.at[:, columns]),
            (block.at[2 * HALF :, :HEAD_WIDTH], next_ref.at[rows, :]),
        ):
            copies.append(pltpu.make_async_copy(source, target, semaphores.at[len(copies)]))
    for copy in copies:
        copy.start()
    for copy in copies:
        copy.wait()


def run_place(where, blocks):
    heads = COLUMNS * HEADS_PER_GROUP
    return pl.pallas_call(
        place,
        out_shape=[
            jax.ShapeDtypeStruct((2 * HALF, COLUMNS * GROUP_WIDTH), jnp.bfloat16),
            jax.ShapeDtypeStruct((heads, HEAD_WIDTH), jnp.bfloat16),
        ],
        in_specs=[pl.BlockSpec(memory_space=pltpu.SMEM)] + [pl.BlockSpec(memory_space=pltpu.VMEM)] * COLUMNS,
        out_specs=[pl.BlockSpec(memory_space=pltpu.HBM)] * 2,
        scratch_shapes=[pltpu.SemaphoreType.DMA((2 * COLUMNS,))],
        compiler_params=pltpu.CompilerParams(vmem_limit_bytes=8 << 20),
        name="place",
    )(where, *blocks)


def rotation(size, by):
    return [(i, (i + by) % size) for i in range(size)]


def body(
    prompt_query,
    prompt_key,
    prompt_value,
    prefix_key_cache,
    prefix_value_cache,
    decoded_query,
    decoded_key,
    decoded_value,
    shard_counts,
    block_offsets,
):
    depth = lax.axis_size("ctx_1")
    x, z, core = (lax.axis_index(a) for a in CTX)
    where = jnp.stack([x, z, core, jnp.zeros_like(x)]).astype(jnp.int32)
    offsets = block_offsets.reshape(-1)
    counts = shard_counts.reshape(-1)

    def key_value_of(head):
        wide = (2 * HALF + PREFIX, 2 * HEAD_WIDTH)
        slots = lax.broadcasted_iota(jnp.int32, wide, 0) < 2 * HALF
        as_key = lax.broadcasted_iota(jnp.int32, wide, 1) < HEAD_WIDTH

        def padded(array, row, column):
            part = lax.dynamic_slice_in_dim(array, head * HEAD_WIDTH, HEAD_WIDTH, 1)
            rows = (row, wide[0] - row - part.shape[0])
            return jnp.pad(part, (rows, (column, wide[1] - column - HEAD_WIDTH)))

        return jnp.where(
            slots,
            jnp.where(as_key, padded(prompt_key, 0, 0), padded(prompt_value, 0, HEAD_WIDTH)),
            jnp.where(
                as_key,
                padded(prefix_key_cache, 2 * HALF, 0),
                padded(prefix_value_cache, 2 * HALF, HEAD_WIDTH),
            ),
        )

    def heads_at(by):
        return lax.rem(x + by, COLUMNS)

    parts = [key_value_of(x)]
    for by in range(1, COLUMNS):
        parts.append(lax.ppermute(key_value_of(heads_at(by)), "ctx_0", rotation(COLUMNS, by)))

    def query_of(head):
        return lax.dynamic_slice_in_dim(prompt_query, head * GROUP_WIDTH, GROUP_WIDTH, 1)

    queries = [query_of(x)]
    for by in range(1, COLUMNS):
        mine = query_of(heads_at(by))
        queries.append(lax.ppermute(mine, "ctx_0", rotation(COLUMNS, by)))

    own = jnp.concatenate(
        [p[:HALF] for p in parts] + [p[2 * HALF :] for p in parts] + [p[HALF : 2 * HALF] for p in parts],
        0,
    )
    query = jnp.stack(queries)

    def to_rows(vector, rows):
        part = lax.dynamic_slice_in_dim(vector.reshape(COLUMNS, -1), x, 1, 0)
        part = part.reshape(-1, HEAD_WIDTH)
        return jnp.concatenate([part, jnp.zeros((rows - part.shape[0], HEAD_WIDTH), part.dtype)], 0)

    decode_query = to_rows(decoded_query, 16)
    decode_key = lax.dynamic_slice_in_dim(decoded_key.reshape(COLUMNS, HEAD_WIDTH), x, 1, 0)
    decode_value = lax.dynamic_slice_in_dim(decoded_value.reshape(COLUMNS, HEAD_WIDTH), x, 1, 0)
    decode = [decode_query, decode_key, decode_value]

    ring = []
    for i in range(depth):
        ring.append((i * CORES, ((i + 1) % depth) * CORES))
        ring.append((i * CORES + 1, ((i - 1) % depth) * CORES + 1))

    def pass_on(block):
        return lax.ppermute(block, RING, ring)

    def swap(block):
        return lax.ppermute(block, "ctx_2", rotation(CORES, 1))

    step = functools.partial(run_step, offsets, counts, depth=depth, query=query, decode=decode)
    near_flips = ((False, False), (False, True))
    far_flips = ((True, True), (True, False))
    first, second = own, swap(own)
    state = None
    for s in range(depth // 2):
        blocks = [first, second]
        if s:
            blocks.append(swap(jnp.concatenate([first, second], 0)))
        state = step(
            where=where,
            blocks=blocks,
            flips=near_flips + far_flips if s else near_flips,
            state=state,
            last=False,
        )
        first = pass_on(first)
        if s + 1 < depth // 2:
            second = pass_on(second)
        where = lax.optimization_barrier(where + jnp.array([0, 0, 0, 1], jnp.int32))
    out = step(
        where=where,
        blocks=[first, swap(first)],
        flips=((False, False), (True, True)),
        state=state,
        last=True,
    )

    back = [out[0]]
    for by in range(1, COLUMNS):
        back.append(lax.ppermute(out[by], "ctx_0", rotation(COLUMNS, -by)))
    span_out, next_out = run_place(where, back)
    return span_out, next_out.reshape(-1)


def solution(mesh):
    groups = mesh.shape["groups"]
    split = Mesh(
        mesh.devices.reshape(groups, COLUMNS, -1, CORES), ("groups", *CTX)
    )

    return jax.shard_map(
        body,
        mesh=split,
        in_specs=(
            P(GROUPS_CTX, None),
            P(GROUPS_CTX, None),
            P(GROUPS_CTX, None),
            P(GROUPS_CTX, None),
            P(GROUPS_CTX, None),
            P("groups"),
            P("groups"),
            P("groups"),
            P("groups", None),
            P("groups", None),
        ),
        out_specs=(P(GROUPS_CTX, None), P("groups")),
        check_vma=False,
    )
```
